32 devices in a mesh: blk: 16 (over z, x, core), dp: 2 (over y).
Axes of the slice: x: 2, y: 2, z: 4, core: 2. Of those that a mesh axis runs over, the one named last changes fastest.
Arguments:
- inputs: bfloat16 [4096, 1024], P(('blk', 'dp')), may hold values from -6 to 6
- cotangent: bfloat16 [4096, 1024], P(('blk', 'dp')), may hold values from -2.5 to 2.5
- task_ids: int32 [4096], P(('blk', 'dp')), may hold values from 0 to 3
- group_counts: int32 [32, 8], P(('blk', 'dp')), may hold values from 1 to 16, as said below
- task_gate: float32 [4, 16], replicated, may hold values from 0.25 to 2
- w_in: bfloat16 [16, 1024, 2048], P('blk'), may hold values from -0.1875 to 0.1875
- w_out: bfloat16 [16, 2048, 1024], P('blk'), may hold values from -0.125 to 0.125
Outputs:
- input_grad: float32 [4096, 1024], P(('blk', 'dp'))
- grad_in: float32 [16, 1024, 2048], P('blk', 'dp')
- grad_out: float32 [16, 2048, 1024], P('blk', 'dp')
The draws below stay inside these ranges and needn't reach their ends.
Inputs may be any that keep to these rules, and one draw needn't show every extreme that they name: `group_counts`: in every draw one group has all 16 slots live on every device; the others vary from device to device.
All inputs are finite; a program needn't handle non-finite values.
Results may differ from the reference program's by a relative error of at most 0.0042.
Values may be sent and summed in bfloat16 or wider, within the bound.
A program may use at most 128 MiB of HBM per device.

```python
import math
import jax
import jax.numpy as jnp
from jax import lax

D = 1024
HW = 2048
GROUPS = 8
TASKS = 4
CAP = 16
EXPERTS = 16
SOURCES = 32
SAMPLES = 4096


def draw_group_counts(key, part):
    key_level = jax.random.fold_in(key, 11)
    key_raw = jax.random.fold_in(key, 12)
    key_full = jax.random.fold_in(key, 13)
    level = jax.random.randint(key_level, (GROUPS,), max(1, CAP // 4), CAP + 1)
    raw_values = jax.random.randint(key_raw, (SOURCES, GROUPS), 0, 1 << 20)
    counts = 1 + raw_values % level[None, :]
    full_group = jax.random.randint(key_full, (), 0, GROUPS)
    filled = jnp.where(jnp.arange(GROUPS)[None, :] == full_group, CAP, counts)
    return filled.astype(jnp.int32)


def with_ends(entries, rng, smallest, high):
    longest = entries.shape.index(max(entries.shape))
    spots = []
    for shift in (0, 1):
        where = [jax.random.randint(jax.random.fold_in(rng, axis), (), 0, length) for axis, length in enumerate(entries.shape)]
        where[longest] = (where[longest] + shift) % entries.shape[longest]
        spots.append(tuple(where))
    return entries.at[spots[0]].set(smallest).at[spots[1]].set(high)


def level_of(stream_key, dims, cuts, least, high):
    loudness = 1.0
    for dim, shards_of in cuts:
        steps = jax.random.uniform(jax.random.fold_in(jax.random.fold_in(stream_key, 6), dim), (shards_of,), jnp.float32, least / len(cuts), high / len(cuts))
        loudness = loudness * jnp.repeat(jnp.exp(steps), dims[dim] // shards_of).reshape((-1,) + (1,) * (len(dims) - 1 - dim))
    return loudness


def noise(key, dims, deviation, limit, shards=(), kind=jnp.bfloat16):
    level = level_of(key, dims, shards, -0.22, 0.18) if shards else 1.0
    drawn = jax.random.normal(key, dims, jnp.float32) * deviation * level
    return jnp.minimum(jnp.maximum(drawn, -limit), limit).astype(kind)


def setup_inputs(seed: int = 0) -> dict:
    key_list = jax.random.split(jax.random.key(seed), 8)
    return {
        "inputs": noise(key_list[0], (SAMPLES, D), 1.0, 6.0, ((0, 32),)),
        "cotangent": noise(key_list[1], (SAMPLES, D), 0.35, 2.5, ((0, 32),)),
        "task_ids": with_ends(jax.random.randint(key_list[2], (SAMPLES,), 0, TASKS), jax.random.fold_in(key_list[2], 1), 0, TASKS - 1).astype(jnp.int32),
        "group_counts": draw_group_counts(jax.random.fold_in(key_list[7], 71), 0),
        "task_gate": jnp.clip(jnp.exp(jax.random.uniform(key_list[4], (TASKS, EXPERTS), jnp.float32, math.log(0.25), math.log(2.0))), 0.25, 2.0),
        "w_in": noise(key_list[5], (EXPERTS, D, HW), D ** -0.5, 0.1875, ((0, 16),)),
        "w_out": noise(key_list[6], (EXPERTS, HW, D), HW ** -0.5, 0.125, ((0, 16),)),
    }


grad_scale = 0.0625


def reference(inputs, cotangent, task_ids, group_counts, task_gate, w_in, w_out):
    inputs_four = inputs.reshape(SOURCES, GROUPS, CAP, D)
    cot_four = cotangent.reshape(SOURCES, GROUPS, CAP, D)
    task_three = task_ids.reshape(SOURCES, GROUPS, CAP)
    slot_index = jnp.arange(CAP, dtype=jnp.int32)
    live_three = slot_index[None, None, :] < group_counts[:, :, None]

    def per_expert(accum, expert):
        group = (expert % GROUPS).astype(jnp.int32)
        x_rows = lax.dynamic_index_in_dim(inputs_four, group, 1, keepdims=False).reshape(SOURCES * CAP, D)
        cot_rows = lax.dynamic_index_in_dim(cot_four, group, 1, keepdims=False).reshape(SOURCES * CAP, D)
        task_rows = lax.dynamic_index_in_dim(task_three, group, 1, keepdims=False).reshape(SOURCES * CAP)
        live_rows = lax.dynamic_index_in_dim(live_three, group, 1, keepdims=False).reshape(SOURCES * CAP)
        column = lax.dynamic_index_in_dim(task_gate, expert.astype(jnp.int32), 1, keepdims=False)
        row_gate = jnp.where(live_rows, column[task_rows], jnp.zeros((), task_gate.dtype)).astype(jnp.float32)
        first_weight = lax.dynamic_index_in_dim(w_in, expert.astype(jnp.int32), 0, keepdims=False)
        second_weight = lax.dynamic_index_in_dim(w_out, expert.astype(jnp.int32), 0, keepdims=False)
        pre_act = jnp.dot(x_rows, first_weight, preferred_element_type=jnp.float32)
        sigmoid_act = jax.nn.sigmoid(pre_act)
        hidden = (pre_act * sigmoid_act).astype(jnp.bfloat16)
        scaled_cot = (row_gate[:, None] * cot_rows.astype(jnp.float32)).astype(jnp.bfloat16)
        hidden_cot = jnp.dot(scaled_cot, second_weight.T, preferred_element_type=jnp.float32)
        pre_cot = (hidden_cot * sigmoid_act * (1.0 + pre_act * (1.0 - sigmoid_act))).astype(jnp.bfloat16)
        grad_second = jnp.dot(hidden.T, scaled_cot, preferred_element_type=jnp.float32) * grad_scale
        grad_first = jnp.dot(x_rows.T, pre_cot, preferred_element_type=jnp.float32) * grad_scale
        row_grad = jnp.dot(pre_cot, first_weight.T, preferred_element_type=jnp.float32)
        current = lax.dynamic_index_in_dim(accum, group, 1, keepdims=False)
        accum = lax.dynamic_update_index_in_dim(accum, current + row_grad.reshape(SOURCES, CAP, D), group, 1)
        return accum, (grad_first, grad_second)

    start = jnp.zeros((SOURCES, GROUPS, CAP, D), jnp.float32)
    accum, stacked = lax.scan(per_expert, start, jnp.arange(EXPERTS, dtype=jnp.int32))
    return accum.reshape(SAMPLES, D), stacked[0], stacked[1]
```

```python
import functools

import jax
import jax.numpy as jnp
from jax import lax
from jax.experimental import pallas as pl
from jax.experimental.pallas import tpu as pltpu
from jax.sharding import PartitionSpec as P

grad_scale = 0.0625
LANES = 128
MESH = pl.DeviceIdType.MESH


def exchange_kernel(
    n, peers, groups, cap, width, hidden, tasks,
    gate_ref, pay_ref, w1_hbm, w2_hbm,
    xh_out, sc_out, act_out, pc_out, home_out,
    buf, w1, w2, sc, act, pc, ret, home,
    send1, recv1, send2, recv2, send3, recv3, local_sem, out_sem,
):
    b = lax.axis_index("blk")
    h = lax.axis_index("dp")
    plane = n * cap
    half_slots = n // 2
    half_rows = half_slots * cap
    width_part = width // peers
    hidden_part = hidden // peers
    tile = 256
    tiles = hidden // tile
    part_tiles = hidden_part // tile

    def offset(i):
        odd = lax.rem(i, 2)
        return odd * ((i + 1) // 2) + (1 - odd) * lax.rem(n - i // 2, n)

    barrier = pltpu.get_barrier_semaphore()

    @pl.loop(1, n)
    def _(k):
        pl.semaphore_signal(barrier, inc=1, device_id=(lax.rem(b + k, n), h), device_id_type=MESH)

    for j in range(1, peers):
        pl.semaphore_signal(barrier, inc=1, device_id=(b, lax.rem(h + j, peers)), device_id_type=MESH)

    get_w1 = pltpu.make_async_copy(w1_hbm.at[0], w1, local_sem.at[0])
    get_w2 = pltpu.make_async_copy(w2_hbm.at[0], w2, local_sem.at[1])
    get_w1.start()
    get_w2.start()
    own = pltpu.make_async_copy(pay_ref.at[lax.rem(b, groups)], buf.at[0, pl.ds(0, cap)], local_sem.at[2])
    own.start()
    pl.semaphore_wait(barrier, n - 1 + peers - 1)

    def outgoing(i):
        target = lax.rem(b + offset(i), n)
        return pltpu.make_async_remote_copy(
            src_ref=pay_ref.at[lax.rem(target, groups)],
            dst_ref=buf.at[0, pl.ds(pl.multiple_of(i * cap, cap), cap)],
            send_sem=send1.at[i], recv_sem=recv1.at[i],
            device_id=(target, h), device_id_type=MESH,
        )

    def forward(i, j):
        rows = pl.ds(pl.multiple_of(i * cap, cap), cap)
        return pltpu.make_async_remote_copy(
            src_ref=buf.at[0, rows], dst_ref=buf.at[j, rows],
            send_sem=send2.at[j - 1, i], recv_sem=recv2.at[j - 1, i],
            device_id=(b, lax.rem(h + j, peers)), device_id_type=MESH,
        )

    def homeward(i):
        rows = pl.ds(pl.multiple_of(i * cap, cap), cap)
        target = lax.rem(b - offset(i) + n, n)
        return pltpu.make_async_remote_copy(
            src_ref=ret.at[rows], dst_ref=home.at[b],
            send_sem=send3.at[i], recv_sem=recv3.at[i],
            device_id=(target, h), device_id_type=MESH,
        )

    @pl.loop(1, n)
    def _(i):
        outgoing(i).start()

    own.wait()
    for j in range(1, peers):
        forward(0, j).start()

    def pass_on(i):
        outgoing(i).wait_recv()
        for j in range(1, peers):
            forward(i, j).start()

    @pl.loop(1, half_slots)
    def _(i):
        pass_on(i)

    get_w1.wait()
    get_w2.wait()

    def rows_forward(j, first, count, hook):
        rows = pl.ds(first, count)
        flat = pl.ds(j * plane + first, count)
        tag = buf[j, rows, pl.ds(2 * width, LANES)].astype(jnp.float32)
        gate = jnp.zeros_like(tag)
        for t in range(tasks):
            gate = gate + jnp.where(tag == float(t), gate_ref[t], 0.0)
        for c in range(width // LANES):
            cot = buf[j, rows, pl.ds(width + c * LANES, LANES)].astype(jnp.float32)
            sc[flat, pl.ds(c * LANES, LANES)] = (gate * cot).astype(jnp.bfloat16)

        def hidden_tile(q, keep):
            at = lax.rem(h * hidden_part + q * tile, hidden)
            columns = pl.ds(pl.multiple_of(at, tile), tile)
            pre = jnp.dot(
                buf[j, rows, pl.ds(0, width)], w1[:, columns], preferred_element_type=jnp.float32
            )
            sig = jax.nn.sigmoid(pre)
            if keep:
                act[flat, pl.ds(pl.multiple_of(q * tile, tile), tile)] = (pre * sig).astype(jnp.bfloat16)
            cot = lax.dot_general(
                sc[flat, :], w2[columns, :], (((1,), (1,)), ((), ())), preferred_element_type=jnp.float32
            )
            pc[flat, columns] = (cot * (sig * (1.0 + pre * (1.0 - sig)))).astype(jnp.bfloat16)
            hook(q)

        @pl.loop(0, part_tiles)
        def _(q):
            hidden_tile(q, True)

        @pl.loop(part_tiles, tiles)
        def _(q):
            hidden_tile(q, False)

    def rows_home(first, count):
        rows = pl.ds(first, count)

        @pl.loop(0, width // tile)
        def _(d):
            columns = pl.ds(pl.multiple_of(d * tile, tile), tile)
            grad = lax.dot_general(
                pc[rows, :], w1[columns, :], (((1,), (1,)), ((), ())), preferred_element_type=jnp.float32
            )
            ret[rows, columns] = grad.astype(jnp.bfloat16)

    late = n - half_slots
    per_tile = late // tiles

    def hook(q):
        for u in range(per_tile):
            pass_on(half_slots + q * per_tile + u)

    rows_forward(0, 0, half_rows, hook)
    for i in range(half_slots + tiles * per_tile, n):
        pass_on(i)
    rows_home(0, half_rows)
    own_home = pltpu.make_async_copy(ret.at[pl.ds(0, cap)], home.at[b], local_sem.at[3])
    own_home.start()

    @pl.loop(1, half_slots)
    def _(i):
        homeward(i).start()

    rows_forward(0, half_rows, plane - half_rows, lambda q: None)
    rows_home(half_rows, plane - half_rows)

    @pl.loop(half_slots, n)
    def _(i):
        homeward(i).start()

    for j in range(1, peers):
        @pl.loop(0, n)
        def _(i):
            forward(i, j).wait_recv()

        rows_forward(j, 0, plane, lambda q: None)

    x_columns = pl.ds(pl.multiple_of(h * width_part, width_part), width_part)
    stores = [
        pltpu.make_async_copy(sc, sc_out, out_sem.at[0]),
        pltpu.make_async_copy(act, act_out, out_sem.at[1]),
        pltpu.make_async_copy(pc, pc_out, out_sem.at[2]),
    ] + [
        pltpu.make_async_copy(
            buf.at[j, :, x_columns], xh_out.at[pl.ds(j * plane, plane)], out_sem.at[4 + j]
        )
        for j in range(peers)
    ]
    for store in stores:
        store.start()

    own_home.wait()

    @pl.loop(1, n)
    def _(i):
        outgoing(i).wait_send()
        homeward(i).wait_recv()

    put_home = pltpu.make_async_copy(home, home_out, out_sem.at[3])
    put_home.start()

    @pl.loop(1, n)
    def _(i):
        homeward(i).wait_send()

    for j in range(1, peers):
        @pl.loop(0, n)
        def _(i):
            forward(i, j).wait_send()

    for store in stores:
        store.wait()
    put_home.wait()


def on_device(n, peers, inputs, cotangent, task_ids, group_counts, task_gate, w_in, w_out):
    groups = group_counts.shape[1]
    width = inputs.shape[1]
    hidden = w_in.shape[2]
    cap = inputs.shape[0] // groups
    tasks = task_gate.shape[0]
    b = lax.axis_index("blk")
    match = jnp.arange(task_gate.shape[1], dtype=jnp.int32) == b
    gate_column = jnp.sum(jnp.where(match[None, :], task_gate, 0.0), axis=1)
    live = jnp.arange(cap, dtype=jnp.int32)[None, :] < group_counts[0][:, None]
    tags = jnp.where(live, task_ids.reshape(groups, cap), tasks).astype(jnp.bfloat16)
    tag_lanes = jnp.broadcast_to(tags[:, :, None], (groups, cap, LANES))
    payload = jnp.concatenate(
        [inputs.reshape(groups, cap, width), cotangent.reshape(groups, cap, width), tag_lanes], axis=2
    )
    full = 2 * width + LANES
    rows = peers * n * cap
    bf16 = jnp.bfloat16
    shape = jax.ShapeDtypeStruct
    hbm = pl.BlockSpec(memory_space=pl.ANY)
    vmem = pl.BlockSpec(memory_space=pltpu.VMEM)
    xh, sc, act, pc, home = pl.pallas_call(
        functools.partial(exchange_kernel, n, peers, groups, cap, width, hidden, tasks),
        out_shape=(
            shape((rows, width // peers), bf16),
            shape((rows, width), bf16),
            shape((rows, hidden // peers), bf16),
            shape((rows, hidden), bf16),
            shape((n, cap, width), bf16),
        ),
        in_specs=[pl.BlockSpec(memory_space=pltpu.SMEM), vmem, hbm, hbm],
        out_specs=(hbm,) * 5,
        scratch_shapes=[
            pltpu.VMEM((peers, n * cap, full), bf16),
            pltpu.VMEM((width, hidden), bf16),
            pltpu.VMEM((hidden, width), bf16),
            pltpu.VMEM((rows, width), bf16),
            pltpu.VMEM((rows, hidden // peers), bf16),
            pltpu.VMEM((rows, hidden), bf16),
            pltpu.VMEM((n * cap, width), bf16),
            pltpu.VMEM((n, cap, width), bf16),
            pltpu.SemaphoreType.DMA((n,)),
            pltpu.SemaphoreType.DMA((n,)),
            pltpu.SemaphoreType.DMA((peers - 1, n)),
            pltpu.SemaphoreType.DMA((peers - 1, n)),
            pltpu.SemaphoreType.DMA((n,)),
            pltpu.SemaphoreType.DMA((n,)),
            pltpu.SemaphoreType.DMA((4,)),
            pltpu.SemaphoreType.DMA((4 + peers,)),
        ],
        compiler_params=pltpu.CompilerParams(collective_id=0, has_side_effects=True),
    )(gate_column, payload, w_in, w_out)
    turned = (((0,), (0,)), ((), ()))
    first = lax.dot_general(xh, pc, turned, preferred_element_type=jnp.float32) * grad_scale
    second = lax.dot_general(act, sc, turned, preferred_element_type=jnp.float32) * grad_scale
    repeats = n // groups
    input_grad = jnp.sum(home.reshape(repeats, groups * cap, width).astype(jnp.float32), axis=0)
    return input_grad, first[None], second[None]


def solution(mesh):
    in_specs = (
        P(("blk", "dp"), None),
        P(("blk", "dp"), None),
        P(("blk", "dp")),
        P(("blk", "dp"), None),
        P(),
        P("blk", None, None),
        P("blk", None, None),
    )
    out_specs = (P(("blk", "dp"), None), P("blk", "dp", None), P("blk", "dp", None))
    body = functools.partial(on_device, mesh.shape["blk"], mesh.shape["dp"])
    return jax.shard_map(body, mesh=mesh, in_specs=in_specs, out_specs=out_specs, check_vma=False)
```

```python
import functools

import jax
import jax.numpy as jnp
from jax import lax
from jax.experimental import pallas as pl
from jax.experimental.pallas import tpu as pltpu
from jax.sharding import PartitionSpec as P

grad_scale = 0.0625
VMEM_BYTES = 40 * 1024 * 1024
MESH = pl.DeviceIdType.MESH


def exchange_kernel(
    n, peers, groups, cap, width, hidden, tasks,
    counts_ref, gate_ref, ids_ref, x_hbm, cot_hbm, w1_hbm, w2_hbm,
    xh, sc, act, pc, home,
    pay, tag, buf, tags, w1, w2, ret,
    send1, recv1, send2, recv2, send3, recv3, tag_send, tag_recv, tag_pass, tag_take, local_sem,
):
    b = lax.axis_index("blk")
    h = lax.axis_index("dp")
    plane = n * cap
    half, quarter = n // 2, n // 4
    width_part = width // peers
    hidden_part = hidden // peers
    tile = 256
    tiles = hidden // tile
    part_tiles = hidden_part // tile
    side, place = b // half, lax.rem(b, half)
    step, spot = place // quarter, lax.rem(place, quarter)
    own_group = lax.rem(b, groups)

    def near_target(i):
        return side * half + lax.rem(place - i + half, half)

    def far_target(i):
        return (1 - side) * half + (i // quarter) * quarter + lax.rem(spot - lax.rem(i, quarter) + quarter, quarter)

    def far_slot(i):
        return half + lax.rem(step + side + 1, 2) * quarter + lax.rem(i, quarter)

    def near_source(i):
        return side * half + lax.rem(place + i, half)

    def far_source(i):
        far = i - half
        ring = far // quarter
        return (1 - side) * half + lax.rem(side + ring, 2) * quarter + lax.rem(spot + lax.rem(far, quarter), quarter)

    def slot_rows(i):
        return pl.ds(pl.multiple_of(i * cap, cap), cap)

    barrier = pltpu.get_barrier_semaphore()

    @pl.loop(1, n)
    def _(k):
        pl.semaphore_signal(barrier, inc=1, device_id=(lax.rem(b + k, n), h), device_id_type=MESH)

    for j in range(1, peers):
        pl.semaphore_signal(barrier, inc=1, device_id=(b, lax.rem(h + j, peers)), device_id_type=MESH)

    get_x = pltpu.make_async_copy(x_hbm, pay.at[:, :, pl.ds(0, width)], local_sem.at[0])
    get_cot = pltpu.make_async_copy(cot_hbm, pay.at[:, :, pl.ds(width, width)], local_sem.at[1])
    get_x.start()
    get_cot.start()

    lane = lax.broadcasted_iota(jnp.int32, tag.shape, 1)
    limit = jnp.zeros(tag.shape, jnp.int32)
    for g in range(groups):
        limit = jnp.where(lane // cap == g, counts_ref[0, g] + g * cap, limit)
    tag[...] = jnp.where(lane < limit, ids_ref[...], tasks).astype(jnp.float32)
    tags[0, 0] = tag[...]

    get_x.wait()
    get_cot.wait()
    own = pltpu.make_async_copy(pay.at[own_group], buf.at[0, pl.ds(0, cap)], local_sem.at[2])
    own.start()
    get_w1 = pltpu.make_async_copy(w1_hbm.at[0], w1, local_sem.at[3])
    get_w2 = pltpu.make_async_copy(w2_hbm.at[0], w2, local_sem.at[4])
    get_w1.start()
    get_w2.start()
    pl.semaphore_wait(barrier, n - 1 + peers - 1)

    def block_out(target, at, slot):
        return pltpu.make_async_remote_copy(
            src_ref=pay.at[lax.rem(target, groups)], dst_ref=buf.at[0, slot_rows(slot)],
            send_sem=send1.at[at], recv_sem=recv1.at[slot],
            device_id=(target, h), device_id_type=MESH,
        )

    def tag_out(target, at, slot):
        return pltpu.make_async_remote_copy(
            src_ref=tag, dst_ref=tags.at[0, slot],
            send_sem=tag_send.at[at], recv_sem=tag_recv.at[slot],
            device_id=(target, h), device_id_type=MESH,
        )

    def tags_on(j):
        return pltpu.make_async_remote_copy(
            src_ref=tags.at[0], dst_ref=tags.at[j],
            send_sem=tag_pass.at[j - 1], recv_sem=tag_take.at[j - 1],
            device_id=(b, lax.rem(h + j, peers)), device_id_type=MESH,
        )

    def forward(i, j):
        return pltpu.make_async_remote_copy(
            src_ref=buf.at[0, slot_rows(i)], dst_ref=buf.at[j, slot_rows(i)],
            send_sem=send2.at[j - 1, i], recv_sem=recv2.at[j - 1, i],
            device_id=(b, lax.rem(h + j, peers)), device_id_type=MESH,
        )

    def homeward(i, target):
        return pltpu.make_async_remote_copy(
            src_ref=ret.at[slot_rows(i)], dst_ref=home.at[b],
            send_sem=send3.at[i], recv_sem=recv3.at[b],
            device_id=(target, h), device_id_type=MESH,
        )

    def home_from(source):
        return pltpu.make_async_remote_copy(
            src_ref=ret.at[slot_rows(0)], dst_ref=home.at[source],
            send_sem=send3.at[0], recv_sem=recv3.at[source],
            device_id=(source, h), device_id_type=MESH,
        )

    @pl.loop(1, half)
    def _(i):
        tag_out(near_target(i), i, i).start()
        block_out(near_target(i), i, i).start()

    @pl.loop(0, half)
    def _(i):
        tag_out(far_target(i), half + i, far_slot(i)).start()
        block_out(far_target(i), half + i, far_slot(i)).start()

    own.wait()
    for j in range(1, peers):
        forward(0, j).start()

    def pass_on(i):
        block_out(near_target(0), i, i).wait_recv()
        for j in range(1, peers):
            forward(i, j).start()

    @pl.loop(1, half)
    def _(i):
        pass_on(i)

    @pl.loop(1, n)
    def _(i):
        tag_out(near_target(0), i, i).wait_recv()

    for j in range(1, peers):
        tags_on(j).start()
    get_w1.wait()
    get_w2.wait()

    def rows_forward(j, slot, count, hook):
        first, total = slot * cap, count * cap
        rows = pl.ds(first, total)
        flat = pl.ds(j * plane + first, total)
        known = tags[j, pl.ds(slot, count)]
        gates = jnp.zeros_like(known)
        for t in range(tasks):
            gates = gates + jnp.where(known == float(t), gate_ref[t, b], 0.0)
        spread = jnp.broadcast_to(gates, (count, cap, groups * cap))
        lanes = lax.broadcasted_iota(jnp.int32, spread.shape, 2)
        places = lax.broadcasted_iota(jnp.int32, spread.shape, 1) + own_group * cap
        gate = jnp.sum(jnp.where(lanes == places, spread, 0.0), axis=2, keepdims=True).reshape(total, 1)
        cot_rows = buf[j, rows, pl.ds(width, width)].astype(jnp.float32)
        sc[flat, :] = (gate * cot_rows).astype(jnp.bfloat16)
        xh[flat, :] = buf[j, rows, pl.ds(pl.multiple_of(h * width_part, width_part), width_part)]

        def hidden_tile(q, keep):
            at = lax.rem(h * hidden_part + q * tile, hidden)
            columns = pl.ds(pl.multiple_of(at, tile), tile)
            pre = jnp.dot(
                buf[j, rows, pl.ds(0, width)], w1[:, columns], preferred_element_type=jnp.float32
            )
            sig = jax.nn.sigmoid(pre)
            if keep:
                act[flat, pl.ds(pl.multiple_of(q * tile, tile), tile)] = (pre * sig).astype(jnp.bfloat16)
            cot = lax.dot_general(
                sc[flat, :], w2[columns, :], (((1,), (1,)), ((), ())), preferred_element_type=jnp.float32
            )
            pc[flat, columns] = (cot * (sig * (1.0 + pre * (1.0 - sig)))).astype(jnp.bfloat16)
            hook(q)

        @pl.loop(0, part_tiles)
        def _(q):
            hidden_tile(q, True)

        @pl.loop(part_tiles, tiles)
        def _(q):
            hidden_tile(q, False)

    def rows_home(slot, count):
        rows = pl.ds(slot * cap, count * cap)

        @pl.loop(0, width // tile)
        def _(d):
            columns = pl.ds(pl.multiple_of(d * tile, tile), tile)
            grad = lax.dot_general(
                pc[rows, :], w1[columns, :], (((1,), (1,)), ((), ())), preferred_element_type=jnp.float32
            )
            ret[rows, columns] = grad.astype(jnp.bfloat16)

    rows_forward(0, 0, half, lambda q: None)
    rows_home(0, half)
    own_home = pltpu.make_async_copy(ret.at[pl.ds(0, cap)], home.at[b], local_sem.at[5])
    own_home.start()

    @pl.loop(1, half)
    def _(i):
        homeward(i, near_source(i)).start()

    for first in (half, half + quarter):
        @pl.loop(first, first + quarter)
        def _(i):
            pass_on(i)

        rows_forward(0, first, quarter, lambda q: None)
        rows_home(first, quarter)

        @pl.loop(first, first + quarter)
        def _(i):
            homeward(i, far_source(i)).start()

    for j in range(1, peers):
        tags_on(j).wait_recv()

        @pl.loop(0, n)
        def _(i):
            forward(i, j).wait_recv()

        rows_forward(j, 0, n, lambda q: None)

    own_home.wait()

    @pl.loop(1, n)
    def _(i):
        block_out(near_target(0), i, i).wait_send()
        tag_out(near_target(0), i, i).wait_send()
        homeward(i, b).wait_send()

    for j in range(1, peers):
        tags_on(j).wait_send()

        @pl.loop(0, n)
        def _(i):
            forward(i, j).wait_send()

    @pl.loop(1, n)
    def _(k):
        home_from(lax.rem(b + k, n)).wait_recv()


def on_device(n, peers, inputs, cotangent, task_ids, group_counts, task_gate, w_in, w_out):
    groups = group_counts.shape[1]
    slots, width = inputs.shape
    hidden = w_in.shape[2]
    cap = slots // groups
    tasks = task_gate.shape[0]
    rows = peers * n * cap
    bf16 = jnp.bfloat16
    hbm = pl.BlockSpec(memory_space=pltpu.HBM)
    smem = pl.BlockSpec(memory_space=pltpu.SMEM)
    vmem = pl.BlockSpec(memory_space=pltpu.VMEM)
    dma = pltpu.SemaphoreType.DMA
    xh, sc, act, pc, home = pl.pallas_call(
        functools.partial(exchange_kernel, n, peers, groups, cap, width, hidden, tasks),
        out_shape=(
            pltpu.VMEM((rows, width // peers), bf16),
            pltpu.VMEM((rows, width), bf16),
            pltpu.VMEM((rows, hidden // peers), bf16),
            pltpu.VMEM((rows, hidden), bf16),
            pltpu.VMEM((n, cap, width), bf16),
        ),
        in_specs=[smem, smem, vmem, hbm, hbm, hbm, hbm],
        out_specs=(vmem,) * 5,
        scratch_shapes=[
            pltpu.VMEM((groups, cap, 2 * width), bf16),
            pltpu.VMEM((1, slots), jnp.float32),
            pltpu.VMEM((peers, n * cap, 2 * width), bf16),
            pltpu.VMEM((peers, n, 1, slots), jnp.float32),
            pltpu.VMEM((width, hidden), bf16),
            pltpu.VMEM((hidden, width), bf16),
            pltpu.VMEM((n * cap, width), bf16),
            dma((n,)), dma((n,)), dma((peers - 1, n)), dma((peers - 1, n)), dma((n,)), dma((n,)),
            dma((n,)), dma((n,)), dma((peers - 1,)), dma((peers - 1,)), dma((6,)),
        ],
        compiler_params=pltpu.CompilerParams(
            collective_id=0, has_side_effects=True, vmem_limit_bytes=VMEM_BYTES
        ),
    )(
        group_counts, task_gate, task_ids.reshape(1, slots),
        *(
            pltpu.with_memory_space_constraint(array, pltpu.HBM)
            for array in (inputs.reshape(groups, cap, width), cotangent.reshape(groups, cap, width), w_in, w_out)
        ),
    )
    turned = (((0,), (0,)), ((), ()))
    first = lax.dot_general(xh, pc, turned, preferred_element_type=jnp.float32) * grad_scale
    second = lax.dot_general(act, sc, turned, preferred_element_type=jnp.float32) * grad_scale
    repeats = n // groups
    input_grad = jnp.sum(home.reshape(repeats, groups * cap, width).astype(jnp.float32), axis=0)
    return input_grad, first[None], second[None]


def solution(mesh):
    in_specs = (
        P(("blk", "dp"), None),
        P(("blk", "dp"), None),
        P(("blk", "dp")),
        P(("blk", "dp"), None),
        P(),
        P("blk", None, None),
        P("blk", None, None),
    )
    out_specs = (P(("blk", "dp"), None), P("blk", "dp", None), P("blk", "dp", None))
    body = functools.partial(on_device, mesh.shape["blk"], mesh.shape["dp"])
    return jax.shard_map(body, mesh=mesh, in_specs=in_specs, out_specs=out_specs, check_vma=False)
```

```python
import functools

import jax
import jax.numpy as jnp
from jax import lax
from jax.experimental import pallas as pl
from jax.experimental.pallas import tpu as pltpu
from jax.sharding import PartitionSpec as P

grad_scale = 0.0625
VMEM_BYTES = 40 * 1024 * 1024
MESH = pl.DeviceIdType.MESH


def exchange_kernel(
    n, peers, groups, cap, width, hidden, tasks,
    counts_hbm, gate_hbm, ids_hbm, x_hbm, cot_hbm, w1_hbm, w2_hbm,
    xh, sc, act, pc, home,
    counts_ref, gate_ref, ids_ref, cots, tag, pay, buf, w1, w2, ret,
    send1, recv1, send2, recv2, send3, recv3, local_sem,
):
    b = lax.axis_index("blk")
    h = lax.axis_index("dp")
    plane = n * cap
    half, quarter = n // 2, n // 4
    width_part = width // peers
    hidden_part = hidden // peers
    tile = 256
    tiles = hidden // tile
    part_tiles = hidden_part // tile
    side, place = b // half, lax.rem(b, half)
    step, spot = place // quarter, lax.rem(place, quarter)

    lead = quarter // 2

    def near_target(i):
        return side * half + lax.rem(place - i + half, half)

    def far_target(i):
        return (1 - side) * half + lax.rem(i, 2) * quarter + lax.rem(spot - i // 2 + quarter, quarter)

    def far_slot(i):
        turn, ring = i // 2, lax.rem(step + side + 1, 2)
        first = jnp.where(turn < lead, turn, 2 * turn - lead)
        second = jnp.where(turn < lead, lead + 2 * turn + 1, quarter + turn)
        return half + jnp.where(ring == 0, first, second)

    def near_source(i):
        return side * half + lax.rem(place + i, half)

    def far_source(i):
        far = i - half
        middle = far - lead
        ring = jnp.where(far < lead, 0, jnp.where(middle < quarter, lax.rem(middle + quarter, 2), 1))
        turn = jnp.where(
            far < lead, far, jnp.where(middle < quarter, middle // 2 + (1 - ring) * lead, far - quarter)
        )
        return (1 - side) * half + lax.rem(side + ring, 2) * quarter + lax.rem(spot + turn, quarter)

    def slot_rows(i):
        return pl.ds(pl.multiple_of(i * cap, cap), cap)

    barrier = pltpu.get_barrier_semaphore()

    @pl.loop(1, n)
    def _(k):
        pl.semaphore_signal(barrier, inc=1, device_id=(lax.rem(b + k, n), h), device_id_type=MESH)

    for j in range(1, peers):
        pl.semaphore_signal(barrier, inc=1, device_id=(b, lax.rem(h + j, peers)), device_id_type=MESH)

    loads = [
        pltpu.make_async_copy(source, target, local_sem.at[6 + at])
        for at, (source, target) in enumerate(
            [(counts_hbm, counts_ref), (gate_hbm, gate_ref), (ids_hbm, ids_ref), (cot_hbm, cots)]
            + [(x_hbm, pay.at[pl.ds(r * groups, groups), :, pl.ds(0, width)]) for r in range(n // groups)]
        )
    ]
    for load in loads:
        load.start()
    get_w1 = pltpu.make_async_copy(w1_hbm.at[0], w1, local_sem.at[3])
    get_w2 = pltpu.make_async_copy(w2_hbm.at[0], w2, local_sem.at[4])
    get_w1.start()
    get_w2.start()
    for load in loads[:4]:
        load.wait()
    slots = groups * cap
    lanes = lax.broadcasted_iota(jnp.int32, (slots, slots), 1)
    places = lax.broadcasted_iota(jnp.int32, (slots, slots), 0)
    ids = jnp.broadcast_to(ids_ref[...].astype(jnp.float32), (slots, slots))
    tag[...] = jnp.broadcast_to(
        jnp.sum(jnp.where(lanes == places, ids, 0.0), axis=1, keepdims=True), tag.shape
    )
    order = lax.broadcasted_iota(jnp.int32, (cap, 1), 0)

    @pl.loop(0, groups)
    def _(g):
        known = tag[slot_rows(g), :][:, 0:1]
        live = order < counts_ref[0, g]
        cot_rows = cots[g].astype(jnp.float32)
        for r in range(n // groups):
            gate = jnp.zeros((cap, 1), jnp.float32)
            for t in range(tasks):
                gate = jnp.where(known == float(t), gate_ref[t, r * groups + g], gate)
            gate = jnp.where(live, gate, 0.0)
            pay[r * groups + g, :, pl.ds(width, width)] = (gate * cot_rows).astype(jnp.bfloat16)

    for load in loads[4:]:
        load.wait()
    own = pltpu.make_async_copy(pay.at[b], buf.at[0, pl.ds(0, cap)], local_sem.at[2])
    own.start()
    pl.semaphore_wait(barrier, n - 1 + peers - 1)

    def block_out(target, at, slot):
        return pltpu.make_async_remote_copy(
            src_ref=pay.at[target], dst_ref=buf.at[0, slot_rows(slot)],
            send_sem=send1.at[at], recv_sem=recv1.at[slot],
            device_id=(target, h), device_id_type=MESH,
        )

    def forward(i, j):
        return pltpu.make_async_remote_copy(
            src_ref=buf.at[0, slot_rows(i)], dst_ref=buf.at[j, slot_rows(i)],
            send_sem=send2.at[j - 1, i], recv_sem=recv2.at[j - 1, i],
            device_id=(b, lax.rem(h + j, peers)), device_id_type=MESH,
        )

    def homeward(i, target):
        return pltpu.make_async_remote_copy(
            src_ref=ret.at[slot_rows(i)], dst_ref=home.at[b],
            send_sem=send3.at[i], recv_sem=recv3.at[b],
            device_id=(target, h), device_id_type=MESH,
        )

    def home_from(source):
        return pltpu.make_async_remote_copy(
            src_ref=ret.at[slot_rows(0)], dst_ref=home.at[source],
            send_sem=send3.at[0], recv_sem=recv3.at[source],
            device_id=(source, h), device_id_type=MESH,
        )

    @pl.loop(1, half)
    def _(i):
        block_out(near_target(i), i, i).start()

    @pl.loop(0, half)
    def _(i):
        block_out(far_target(i), half + i, far_slot(i)).start()

    own.wait()
    for j in range(1, peers):
        forward(0, j).start()

    def pass_on(i):
        block_out(near_target(0), i, i).wait_recv()
        for j in range(1, peers):
            forward(i, j).start()

    @pl.loop(1, half)
    def _(i):
        pass_on(i)

    get_w1.wait()
    get_w2.wait()

    def rows_forward(j, slot, count, hook):
        first, total = slot * cap, count * cap
        rows = pl.ds(first, total)
        flat = pl.ds(j * plane + first, total)
        sc[flat, :] = buf[j, rows, pl.ds(width, width)]
        xh[flat, :] = buf[j, rows, pl.ds(pl.multiple_of(h * width_part, width_part), width_part)]

        def hidden_tile(q, keep):
            at = lax.rem(h * hidden_part + q * tile, hidden)
            columns = pl.ds(pl.multiple_of(at, tile), tile)
            pre = jnp.dot(
                buf[j, rows, pl.ds(0, width)], w1[:, columns], preferred_element_type=jnp.float32
            )
            sig = jax.nn.sigmoid(pre)
            if keep:
                act[flat, pl.ds(pl.multiple_of(q * tile, tile), tile)] = (pre * sig).astype(jnp.bfloat16)
            cot = lax.dot_general(
                buf[j, rows, pl.ds(width, width)], w2[columns, :], (((1,), (1,)), ((), ())), preferred_element_type=jnp.float32
            )
            pc[flat, columns] = (cot * (sig * (1.0 + pre * (1.0 - sig)))).astype(jnp.bfloat16)
            hook(q)

        @pl.loop(0, part_tiles)
        def _(q):
            hidden_tile(q, True)

        @pl.loop(part_tiles, tiles)
        def _(q):
            hidden_tile(q, False)

    def rows_home(slot, count):
        rows = pl.ds(slot * cap, count * cap)

        @pl.loop(0, width // tile)
        def _(d):
            columns = pl.ds(pl.multiple_of(d * tile, tile), tile)
            grad = lax.dot_general(
                pc[rows, :], w1[columns, :], (((1,), (1,)), ((), ())), preferred_element_type=jnp.float32
            )
            ret[rows, columns] = grad.astype(jnp.bfloat16)

    rows_forward(0, 0, half, lambda q: None)
    rows_home(0, half)
    own_home = pltpu.make_async_copy(ret.at[pl.ds(0, cap)], home.at[b], local_sem.at[5])
    own_home.start()

    @pl.loop(1, half)
    def _(i):
        homeward(i, near_source(i)).start()

    for first in (half, half + quarter):
        @pl.loop(first, first + quarter)
        def _(i):
            pass_on(i)

        rows_forward(0, first, quarter, lambda q: None)
        rows_home(first, quarter)

        @pl.loop(first, first + quarter)
        def _(i):
            homeward(i, far_source(i)).start()

    for j in range(1, peers):
        @pl.loop(0, n)
        def _(i):
            forward(i, j).wait_recv()

        rows_forward(j, 0, n, lambda q: None)

    own_home.wait()

    @pl.loop(1, n)
    def _(i):
        block_out(near_target(0), i, i).wait_send()
        homeward(i, b).wait_send()

    for j in range(1, peers):
        @pl.loop(0, n)
        def _(i):
            forward(i, j).wait_send()

    @pl.loop(1, n)
    def _(k):
        home_from(lax.rem(b + k, n)).wait_recv()


def on_device(n, peers, inputs, cotangent, task_ids, group_counts, task_gate, w_in, w_out):
    groups = group_counts.shape[1]
    slots, width = inputs.shape
    hidden = w_in.shape[2]
    cap = slots // groups
    tasks = task_gate.shape[0]
    rows = peers * n * cap
    bf16 = jnp.bfloat16
    hbm = pl.BlockSpec(memory_space=pltpu.HBM)
    vmem = pl.BlockSpec(memory_space=pltpu.VMEM)
    dma = pltpu.SemaphoreType.DMA
    xh, sc, act, pc, home = pl.pallas_call(
        functools.partial(exchange_kernel, n, peers, groups, cap, width, hidden, tasks),
        out_shape=(
            pltpu.VMEM((rows, width // peers), bf16),
            pltpu.VMEM((rows, width), bf16),
            pltpu.VMEM((rows, hidden // peers), bf16),
            pltpu.VMEM((rows, hidden), bf16),
            pltpu.VMEM((n, cap, width), bf16),
        ),
        in_specs=[hbm] * 7,
        out_specs=(vmem,) * 5,
        scratch_shapes=[
            pltpu.SMEM(group_counts.shape, jnp.int32),
            pltpu.SMEM(task_gate.shape, jnp.float32),
            pltpu.VMEM((1, slots), jnp.int32),
            pltpu.VMEM((groups, cap, width), bf16),
            pltpu.VMEM((slots, slots), jnp.float32),
            pltpu.VMEM((n, cap, 2 * width), bf16),
            pltpu.VMEM((peers, n * cap, 2 * width), bf16),
            pltpu.VMEM((width, hidden), bf16),
            pltpu.VMEM((hidden, width), bf16),
            pltpu.VMEM((n * cap, width), bf16),
            dma((n,)), dma((n,)), dma((peers - 1, n)), dma((peers - 1, n)), dma((n,)), dma((n,)),
            dma((10 + n // groups,)),
        ],
        compiler_params=pltpu.CompilerParams(
            collective_id=0, has_side_effects=True, vmem_limit_bytes=VMEM_BYTES
        ),
    )(
        *(
            pltpu.with_memory_space_constraint(array, pltpu.HBM)
            for array in (
                group_counts, task_gate, task_ids.reshape(1, slots), inputs.reshape(groups, cap, width),
                cotangent.reshape(groups, cap, width), w_in, w_out,
            )
        )
    )
    turned = (((0,), (0,)), ((), ()))
    first = lax.dot_general(xh, pc, turned, preferred_element_type=jnp.float32) * grad_scale
    second = lax.dot_general(act, sc, turned, preferred_element_type=jnp.float32) * grad_scale
    repeats = n // groups
    input_grad = jnp.sum(home.reshape(repeats, groups * cap, width).astype(jnp.float32), axis=0)
    return input_grad, first[None], second[None]


def solution(mesh):
    in_specs = (
        P(("blk", "dp"), None),
        P(("blk", "dp"), None),
        P(("blk", "dp")),
        P(("blk", "dp"), None),
        P(),
        P("blk", None, None),
        P("blk", None, None),
    )
    out_specs = (P(("blk", "dp"), None), P("blk", "dp", None), P("blk", "dp", None))
    body = functools.partial(on_device, mesh.shape["blk"], mesh.shape["dp"])
    return jax.shard_map(body, mesh=mesh, in_specs=in_specs, out_specs=out_specs, check_vma=False)
```

```python
import functools

import jax
import jax.numpy as jnp
from jax import lax
from jax.experimental import pallas as pl
from jax.experimental.pallas import tpu as pltpu
from jax.sharding import PartitionSpec as P

grad_scale = 0.0625
VMEM_BYTES = 40 * 1024 * 1024
MESH = pl.DeviceIdType.MESH


def exchange_kernel(
    n, peers, groups, cap, width, hidden, tasks,
    counts_hbm, gate_hbm, ids_hbm, x_hbm, cot_hbm, w1_hbm, w2_hbm,
    xh, sc, act, pc, home,
    counts_ref, gate_ref, ids_ref, cots, tag, pay, buf, w1, w2, ret,
    send1, recv1, send2, recv2, send3, recv3, local_sem,
):
    b = lax.axis_index("blk")
    h = lax.axis_index("dp")
    plane = n * cap
    half, quarter = n // 2, n // 4
    width_part = width // peers
    hidden_part = hidden // peers
    tile = 256
    tiles = hidden // tile
    part_tiles = hidden_part // tile
    side, place = b // half, lax.rem(b, half)
    step, spot = place // quarter, lax.rem(place, quarter)

    def near_target(i):
        return side * half + lax.rem(place - i + half, half)

    def far_target(i):
        return (1 - side) * half + lax.rem(i, 2) * quarter + lax.rem(spot - i // 2 + quarter, quarter)

    def far_slot(i):
        return half + lax.rem(step + side + 1, 2) * quarter + i // 2

    def near_source(i):
        return side * half + lax.rem(place + i, half)

    def far_source(i):
        far = i - half
        ring = far // quarter
        return (1 - side) * half + lax.rem(side + ring, 2) * quarter + lax.rem(spot + lax.rem(far, quarter), quarter)

    def slot_rows(i):
        return pl.ds(pl.multiple_of(i * cap, cap), cap)

    barrier = pltpu.get_barrier_semaphore()

    @pl.loop(1, n)
    def _(k):
        pl.semaphore_signal(barrier, inc=1, device_id=(lax.rem(b + k, n), h), device_id_type=MESH)

    for j in range(1, peers):
        @pl.loop(0, half)
        def _(i):
            pl.semaphore_signal(
                barrier, inc=1, device_id=(near_target(i), lax.rem(h + j, peers)), device_id_type=MESH
            )

    loads = [
        pltpu.make_async_copy(source, target, local_sem.at[6 + at])
        for at, (source, target) in enumerate(
            [(counts_hbm, counts_ref), (gate_hbm, gate_ref), (ids_hbm, ids_ref), (cot_hbm, cots)]
            + [(x_hbm, pay.at[pl.ds(r * groups, groups), :, pl.ds(0, width)]) for r in range(n // groups)]
        )
    ]
    for load in loads:
        load.start()
    get_w1 = pltpu.make_async_copy(w1_hbm.at[0], w1, local_sem.at[3])
    get_w2 = pltpu.make_async_copy(w2_hbm.at[0], w2, local_sem.at[4])
    get_w1.start()
    get_w2.start()
    for load in loads[:4]:
        load.wait()
    slots = groups * cap
    lanes = lax.broadcasted_iota(jnp.int32, (slots, slots), 1)
    places = lax.broadcasted_iota(jnp.int32, (slots, slots), 0)
    ids = jnp.broadcast_to(ids_ref[...].astype(jnp.float32), (slots, slots))
    tag[...] = jnp.broadcast_to(
        jnp.sum(jnp.where(lanes == places, ids, 0.0), axis=1, keepdims=True), tag.shape
    )
    order = lax.broadcasted_iota(jnp.int32, (cap, 1), 0)

    @pl.loop(0, groups)
    def _(g):
        known = tag[slot_rows(g), :][:, 0:1]
        live = order < counts_ref[0, g]
        cot_rows = cots[g].astype(jnp.float32)
        for r in range(n // groups):
            gate = jnp.zeros((cap, 1), jnp.float32)
            for t in range(tasks):
                gate = jnp.where(known == float(t), gate_ref[t, r * groups + g], gate)
            gate = jnp.where(live, gate, 0.0)
            pay[r * groups + g, :, pl.ds(width, width)] = (gate * cot_rows).astype(jnp.bfloat16)

    for load in loads[4:]:
        load.wait()
    own = pltpu.make_async_copy(pay.at[b], buf.at[0, pl.ds(0, cap)], local_sem.at[2])
    own.start()
    pl.semaphore_wait(barrier, n - 1 + (peers - 1) * half)

    def block_out(target, at, slot):
        return pltpu.make_async_remote_copy(
            src_ref=pay.at[target], dst_ref=buf.at[0, slot_rows(slot)],
            send_sem=send1.at[at], recv_sem=recv1.at[slot],
            device_id=(target, h), device_id_type=MESH,
        )

    def across(i, j):
        target = near_target(i)
        return pltpu.make_async_remote_copy(
            src_ref=pay.at[target], dst_ref=buf.at[j, slot_rows(i)],
            send_sem=send2.at[j - 1, i], recv_sem=recv2.at[j - 1, i],
            device_id=(target, lax.rem(h + j, peers)), device_id_type=MESH,
        )

    def forward(i, j):
        return pltpu.make_async_remote_copy(
            src_ref=buf.at[0, slot_rows(i)], dst_ref=buf.at[j, slot_rows(i)],
            send_sem=send2.at[j - 1, i], recv_sem=recv2.at[j - 1, i],
            device_id=(b, lax.rem(h + j, peers)), device_id_type=MESH,
        )

    def homeward(i, target):
        return pltpu.make_async_remote_copy(
            src_ref=ret.at[slot_rows(i)], dst_ref=home.at[b],
            send_sem=send3.at[i], recv_sem=recv3.at[b],
            device_id=(target, h), device_id_type=MESH,
        )

    def home_from(source):
        return pltpu.make_async_remote_copy(
            src_ref=ret.at[slot_rows(0)], dst_ref=home.at[source],
            send_sem=send3.at[0], recv_sem=recv3.at[source],
            device_id=(source, h), device_id_type=MESH,
        )

    for j in range(1, peers):
        across(0, j).start()

    @pl.loop(1, half)
    def _(i):
        block_out(near_target(i), i, i).start()
        for j in range(1, peers):
            across(i, j).start()

    @pl.loop(0, half)
    def _(i):
        block_out(far_target(i), half + i, far_slot(i)).start()

    def pass_on(i):
        block_out(near_target(0), i, i).wait_recv()
        for j in range(1, peers):
            forward(i, j).start()

    early = half + quarter

    @pl.loop(half, early)
    def _(i):
        pass_on(i)

    @pl.loop(1, half)
    def _(i):
        block_out(near_target(0), i, i).wait_recv()

    own.wait()
    get_w1.wait()
    get_w2.wait()

    def rows_forward(j, slot, count, hook):
        first, total = slot * cap, count * cap
        rows = pl.ds(first, total)
        flat = pl.ds(j * plane + first, total)
        sc[flat, :] = buf[j, rows, pl.ds(width, width)]
        xh[flat, :] = buf[j, rows, pl.ds(pl.multiple_of(h * width_part, width_part), width_part)]

        def hidden_tile(q, keep):
            at = lax.rem(h * hidden_part + q * tile, hidden)
            columns = pl.ds(pl.multiple_of(at, tile), tile)
            pre = jnp.dot(
                buf[j, rows, pl.ds(0, width)], w1[:, columns], preferred_element_type=jnp.float32
            )
            sig = jax.nn.sigmoid(pre)
            if keep:
                act[flat, pl.ds(pl.multiple_of(q * tile, tile), tile)] = (pre * sig).astype(jnp.bfloat16)
            cot = lax.dot_general(
                buf[j, rows, pl.ds(width, width)], w2[columns, :], (((1,), (1,)), ((), ())), preferred_element_type=jnp.float32
            )
            pc[flat, columns] = (cot * (sig * (1.0 + pre * (1.0 - sig)))).astype(jnp.bfloat16)
            hook(q)

        @pl.loop(0, part_tiles)
        def _(q):
            hidden_tile(q, True)

        @pl.loop(part_tiles, tiles)
        def _(q):
            hidden_tile(q, False)

    def rows_home(slot, count):
        rows = pl.ds(slot * cap, count * cap)

        @pl.loop(0, width // tile)
        def _(d):
            columns = pl.ds(pl.multiple_of(d * tile, tile), tile)
            grad = lax.dot_general(
                pc[rows, :], w1[columns, :], (((1,), (1,)), ((), ())), preferred_element_type=jnp.float32
            )
            ret[rows, columns] = grad.astype(jnp.bfloat16)

    def partner_rows(j, first, count, hook):
        @pl.loop(first, first + count)
        def _(i):
            forward(i, j).wait_recv()

        rows_forward(j, first, count, hook)

    def late_blocks(q):
        @pl.loop(early + quarter * q // tiles, early + quarter * (q + 1) // tiles)
        def _(i):
            pass_on(i)

    rows_forward(0, 0, early, lambda q: None)
    rows_home(0, early)
    own_home = pltpu.make_async_copy(ret.at[pl.ds(0, cap)], home.at[b], local_sem.at[5])
    own_home.start()

    @pl.loop(half, early)
    def _(i):
        homeward(i, far_source(i)).start()

    @pl.loop(1, half)
    def _(i):
        homeward(i, near_source(i)).start()

    for j in range(1, peers):
        partner_rows(j, 0, half, late_blocks if j == 1 else lambda q: None)

    rows_forward(0, early, n - early, lambda q: None)
    rows_home(early, n - early)

    @pl.loop(early, n)
    def _(i):
        homeward(i, far_source(i)).start()

    for j in range(1, peers):
        partner_rows(j, half, n - half, lambda q: None)

    own_home.wait()

    @pl.loop(1, n)
    def _(i):
        block_out(near_target(0), i, i).wait_send()
        homeward(i, b).wait_send()

    for j in range(1, peers):
        @pl.loop(0, n)
        def _(i):
            forward(i, j).wait_send()

    @pl.loop(1, n)
    def _(k):
        home_from(lax.rem(b + k, n)).wait_recv()


def on_device(n, peers, inputs, cotangent, task_ids, group_counts, task_gate, w_in, w_out):
    groups = group_counts.shape[1]
    slots, width = inputs.shape
    hidden = w_in.shape[2]
    cap = slots // groups
    tasks = task_gate.shape[0]
    rows = peers * n * cap
    bf16 = jnp.bfloat16
    hbm = pl.BlockSpec(memory_space=pltpu.HBM)
    vmem = pl.BlockSpec(memory_space=pltpu.VMEM)
    dma = pltpu.SemaphoreType.DMA
    xh, sc, act, pc, home = pl.pallas_call(
        functools.partial(exchange_kernel, n, peers, groups, cap, width, hidden, tasks),
        out_shape=(
            pltpu.VMEM((rows, width // peers), bf16),
            pltpu.VMEM((rows, width), bf16),
            pltpu.VMEM((rows, hidden // peers), bf16),
            pltpu.VMEM((rows, hidden), bf16),
            pltpu.VMEM((n, cap, width), bf16),
        ),
        in_specs=[hbm] * 7,
        out_specs=(vmem,) * 5,
        scratch_shapes=[
            pltpu.SMEM(group_counts.shape, jnp.int32),
            pltpu.SMEM(task_gate.shape, jnp.float32),
            pltpu.VMEM((1, slots), jnp.int32),
            pltpu.VMEM((groups, cap, width), bf16),
            pltpu.VMEM((slots, slots), jnp.float32),
            pltpu.VMEM((n, cap, 2 * width), bf16),
            pltpu.VMEM((peers, n * cap, 2 * width), bf16),
            pltpu.VMEM((width, hidden), bf16),
            pltpu.VMEM((hidden, width), bf16),
            pltpu.VMEM((n * cap, width), bf16),
            dma((n,)), dma((n,)), dma((peers - 1, n)), dma((peers - 1, n)), dma((n,)), dma((n,)),
            dma((10 + n // groups,)),
        ],
        compiler_params=pltpu.CompilerParams(
            collective_id=0, has_side_effects=True, vmem_limit_bytes=VMEM_BYTES
        ),
    )(
        *(
            pltpu.with_memory_space_constraint(array, pltpu.HBM)
            for array in (
                group_counts, task_gate, task_ids.reshape(1, slots), inputs.reshape(groups, cap, width),
                cotangent.reshape(groups, cap, width), w_in, w_out,
            )
        )
    )
    turned = (((0,), (0,)), ((), ()))
    first = lax.dot_general(xh, pc, turned, preferred_element_type=jnp.float32) * grad_scale
    second = lax.dot_general(act, sc, turned, preferred_element_type=jnp.float32) * grad_scale
    repeats = n // groups
    input_grad = jnp.sum(home.reshape(repeats, groups * cap, width).astype(jnp.float32), axis=0)
    return input_grad, first[None], second[None]


def solution(mesh):
    in_specs = (
        P(("blk", "dp"), None),
        P(("blk", "dp"), None),
        P(("blk", "dp")),
        P(("blk", "dp"), None),
        P(),
        P("blk", None, None),
        P("blk", None, None),
    )
    out_specs = (P(("blk", "dp"), None), P("blk", "dp", None), P("blk", "dp", None))
    body = functools.partial(on_device, mesh.shape["blk"], mesh.shape["dp"])
    return jax.shard_map(body, mesh=mesh, in_specs=in_specs, out_specs=out_specs, check_vma=False)
```

```python
import functools

import jax
import jax.numpy as jnp
from jax import lax
from jax.experimental import pallas as pl
from jax.experimental.pallas import tpu as pltpu
from jax.sharding import PartitionSpec as P

grad_scale = 0.0625
VMEM_BYTES = 40 * 1024 * 1024
MESH = pl.DeviceIdType.MESH


def exchange_kernel(
    n, peers, groups, cap, width, hidden, tasks,
    counts_hbm, gate_hbm, ids_hbm, x_hbm, cot_hbm, w1_hbm, w2_hbm,
    xh, sc, act, pc, home,
    counts_ref, gate_ref, ids_ref, cots, tag, pay, buf, w1, w2, ret,
    send1, recv1, send2, recv2, send3, recv3, local_sem,
):
    b = lax.axis_index("blk")
    h = lax.axis_index("dp")
    plane = n * cap
    half, quarter = n // 2, n // 4
    width_part = width // peers
    hidden_part = hidden // peers
    tile = 512
    tiles = hidden // tile
    part_tiles = hidden_part // tile
    side, place = b // half, lax.rem(b, half)
    step, spot = place // quarter, lax.rem(place, quarter)

    def near_target(i):
        return side * half + lax.rem(place - i + half, half)

    def far_target(i):
        return (1 - side) * half + lax.rem(i, 2) * quarter + lax.rem(spot - i // 2 + quarter, quarter)

    def far_slot(i):
        return half + lax.rem(step + side + 1, 2) * quarter + i // 2

    def near_source(i):
        return side * half + lax.rem(place + i, half)

    def far_source(i):
        far = i - half
        ring = far // quarter
        return (1 - side) * half + lax.rem(side + ring, 2) * quarter + lax.rem(spot + lax.rem(far, quarter), quarter)

    def slot_rows(i):
        return pl.ds(pl.multiple_of(i * cap, cap), cap)

    barrier = pltpu.get_barrier_semaphore()

    @pl.loop(1, n)
    def _(k):
        pl.semaphore_signal(barrier, inc=1, device_id=(lax.rem(b + k, n), h), device_id_type=MESH)

    for j in range(1, peers):
        @pl.loop(0, half)
        def _(i):
            pl.semaphore_signal(
                barrier, inc=1, device_id=(near_target(i), lax.rem(h + j, peers)), device_id_type=MESH
            )

    loads = [
        pltpu.make_async_copy(source, target, local_sem.at[6 + at])
        for at, (source, target) in enumerate(
            [(counts_hbm, counts_ref), (gate_hbm, gate_ref), (ids_hbm, ids_ref), (cot_hbm, cots)]
            + [(x_hbm, pay.at[pl.ds(r * groups, groups), :, pl.ds(0, width)]) for r in range(n // groups)]
        )
    ]
    for load in loads:
        load.start()
    get_w1 = pltpu.make_async_copy(w1_hbm.at[0], w1, local_sem.at[3])
    get_w2 = pltpu.make_async_copy(w2_hbm.at[0], w2, local_sem.at[4])
    get_w1.start()
    get_w2.start()
    for load in loads[:4]:
        load.wait()
    slots = groups * cap
    lanes = lax.broadcasted_iota(jnp.int32, (slots, slots), 1)
    places = lax.broadcasted_iota(jnp.int32, (slots, slots), 0)
    ids = jnp.broadcast_to(ids_ref[...].astype(jnp.float32), (slots, slots))
    tag[...] = jnp.broadcast_to(
        jnp.sum(jnp.where(lanes == places, ids, 0.0), axis=1, keepdims=True), tag.shape
    )
    order = lax.broadcasted_iota(jnp.int32, (cap, 1), 0)

    @pl.loop(0, groups)
    def _(g):
        known = tag[slot_rows(g), :][:, 0:1]
        live = order < counts_ref[0, g]
        cot_rows = cots[g].astype(jnp.float32)
        for r in range(n // groups):
            gate = jnp.zeros((cap, 1), jnp.float32)
            for t in range(tasks):
                gate = jnp.where(known == float(t), gate_ref[t, r * groups + g], gate)
            gate = jnp.where(live, gate, 0.0)
            pay[r * groups + g, :, pl.ds(width, width)] = (gate * cot_rows).astype(jnp.bfloat16)

    for load in loads[4:]:
        load.wait()
    own = pltpu.make_async_copy(pay.at[b], buf.at[0, pl.ds(0, cap)], local_sem.at[2])
    own.start()
    pl.semaphore_wait(barrier, n - 1 + (peers - 1) * half)

    def block_out(target, at, slot):
        return pltpu.make_async_remote_copy(
            src_ref=pay.at[target], dst_ref=buf.at[0, slot_rows(slot)],
            send_sem=send1.at[at], recv_sem=recv1.at[slot],
            device_id=(target, h), device_id_type=MESH,
        )

    def across(i, j):
        target = near_target(i)
        return pltpu.make_async_remote_copy(
            src_ref=pay.at[target], dst_ref=buf.at[j, slot_rows(i)],
            send_sem=send2.at[j - 1, i], recv_sem=recv2.at[j - 1, i],
            device_id=(target, lax.rem(h + j, peers)), device_id_type=MESH,
        )

    def forward(i, j):
        return pltpu.make_async_remote_copy(
            src_ref=buf.at[0, slot_rows(i)], dst_ref=buf.at[j, slot_rows(i)],
            send_sem=send2.at[j - 1, i], recv_sem=recv2.at[j - 1, i],
            device_id=(b, lax.rem(h + j, peers)), device_id_type=MESH,
        )

    def homeward(i, target):
        return pltpu.make_async_remote_copy(
            src_ref=ret.at[slot_rows(i)], dst_ref=home.at[b],
            send_sem=send3.at[i], recv_sem=recv3.at[b],
            device_id=(target, h), device_id_type=MESH,
        )

    def home_from(source):
        return pltpu.make_async_remote_copy(
            src_ref=ret.at[slot_rows(0)], dst_ref=home.at[source],
            send_sem=send3.at[0], recv_sem=recv3.at[source],
            device_id=(source, h), device_id_type=MESH,
        )

    for j in range(1, peers):
        across(0, j).start()

    @pl.loop(1, half)
    def _(i):
        block_out(near_target(i), i, i).start()
        for j in range(1, peers):
            across(i, j).start()

    @pl.loop(0, half)
    def _(i):
        block_out(far_target(i), half + i, far_slot(i)).start()

    def pass_on(i):
        block_out(near_target(0), i, i).wait_recv()
        for j in range(1, peers):
            forward(i, j).start()

    early = half + quarter

    @pl.loop(half, early)
    def _(i):
        pass_on(i)

    @pl.loop(1, half)
    def _(i):
        block_out(near_target(0), i, i).wait_recv()

    own.wait()
    get_w1.wait()
    get_w2.wait()

    def rows_forward(j, slot, count, hook):
        first, total = slot * cap, count * cap
        rows = pl.ds(first, total)
        flat = pl.ds(j * plane + first, total)
        sc[flat, :] = buf[j, rows, pl.ds(width, width)]
        xh[flat, :] = buf[j, rows, pl.ds(pl.multiple_of(h * width_part, width_part), width_part)]

        def hidden_tile(q, keep):
            at = lax.rem(h * hidden_part + q * tile, hidden)
            columns = pl.ds(pl.multiple_of(at, tile), tile)
            pre = jnp.dot(
                buf[j, rows, pl.ds(0, width)], w1[:, columns], preferred_element_type=jnp.float32
            )
            sig = jax.nn.sigmoid(pre)
            if keep:
                act[flat, pl.ds(pl.multiple_of(q * tile, tile), tile)] = (pre * sig).astype(jnp.bfloat16)
            cot = lax.dot_general(
                buf[j, rows, pl.ds(width, width)], w2[columns, :], (((1,), (1,)), ((), ())), preferred_element_type=jnp.float32
            )
            pc[flat, columns] = (cot * (sig * (1.0 + pre * (1.0 - sig)))).astype(jnp.bfloat16)
            hook(q)

        @pl.loop(0, part_tiles)
        def _(q):
            hidden_tile(q, True)

        @pl.loop(part_tiles, tiles)
        def _(q):
            hidden_tile(q, False)

    def rows_home(slot, count):
        rows = pl.ds(slot * cap, count * cap)

        @pl.loop(0, width // tile)
        def _(d):
            columns = pl.ds(pl.multiple_of(d * tile, tile), tile)
            grad = lax.dot_general(
                pc[rows, :], w1[columns, :], (((1,), (1,)), ((), ())), preferred_element_type=jnp.float32
            )
            ret[rows, columns] = grad.astype(jnp.bfloat16)

    def partner_rows(j, first, count, hook):
        @pl.loop(first, first + count)
        def _(i):
            forward(i, j).wait_recv()

        rows_forward(j, first, count, hook)

    rows_forward(0, 0, early, lambda q: None)
    rows_home(0, early)
    own_home = pltpu.make_async_copy(ret.at[pl.ds(0, cap)], home.at[b], local_sem.at[5])
    own_home.start()

    @pl.loop(half, early)
    def _(i):
        homeward(i, far_source(i)).start()

    @pl.loop(1, half)
    def _(i):
        homeward(i, near_source(i)).start()

    @pl.loop(early, n)
    def _(i):
        pass_on(i)

    rows_forward(0, early, n - early, lambda q: None)
    rows_home(early, n - early)

    @pl.loop(early, n)
    def _(i):
        homeward(i, far_source(i)).start()

    for j in range(1, peers):
        partner_rows(j, 0, n, lambda q: None)

    own_home.wait()

    @pl.loop(1, n)
    def _(i):
        block_out(near_target(0), i, i).wait_send()
        homeward(i, b).wait_send()

    for j in range(1, peers):
        @pl.loop(0, n)
        def _(i):
            forward(i, j).wait_send()

    @pl.loop(1, n)
    def _(k):
        home_from(lax.rem(b + k, n)).wait_recv()


def on_device(n, peers, inputs, cotangent, task_ids, group_counts, task_gate, w_in, w_out):
    groups = group_counts.shape[1]
    slots, width = inputs.shape
    hidden = w_in.shape[2]
    cap = slots // groups
    tasks = task_gate.shape[0]
    rows = peers * n * cap
    bf16 = jnp.bfloat16
    hbm = pl.BlockSpec(memory_space=pltpu.HBM)
    vmem = pl.BlockSpec(memory_space=pltpu.VMEM)
    dma = pltpu.SemaphoreType.DMA
    xh, sc, act, pc, home = pl.pallas_call(
        functools.partial(exchange_kernel, n, peers, groups, cap, width, hidden, tasks),
        out_shape=(
            pltpu.VMEM((rows, width // peers), bf16),
            pltpu.VMEM((rows, width), bf16),
            pltpu.VMEM((rows, hidden // peers), bf16),
            pltpu.VMEM((rows, hidden), bf16),
            pltpu.VMEM((n, cap, width), bf16),
        ),
        in_specs=[hbm] * 7,
        out_specs=(vmem,) * 5,
        scratch_shapes=[
            pltpu.SMEM(group_counts.shape, jnp.int32),
            pltpu.SMEM(task_gate.shape, jnp.float32),
            pltpu.VMEM((1, slots), jnp.int32),
            pltpu.VMEM((groups, cap, width), bf16),
            pltpu.VMEM((slots, slots), jnp.float32),
            pltpu.VMEM((n, cap, 2 * width), bf16),
            pltpu.VMEM((peers, n * cap, 2 * width), bf16),
            pltpu.VMEM((width, hidden), bf16),
            pltpu.VMEM((hidden, width), bf16),
            pltpu.VMEM((n * cap, width), bf16),
            dma((n,)), dma((n,)), dma((peers - 1, n)), dma((peers - 1, n)), dma((n,)), dma((n,)),
            dma((10 + n // groups,)),
        ],
        compiler_params=pltpu.CompilerParams(
            collective_id=0, has_side_effects=True, vmem_limit_bytes=VMEM_BYTES
        ),
    )(
        *(
            pltpu.with_memory_space_constraint(array, pltpu.HBM)
            for array in (
                group_counts, task_gate, task_ids.reshape(1, slots), inputs.reshape(groups, cap, width),
                cotangent.reshape(groups, cap, width), w_in, w_out,
            )
        )
    )
    turned = (((0,), (0,)), ((), ()))
    first = lax.dot_general(xh, pc, turned, preferred_element_type=jnp.float32) * grad_scale
    second = lax.dot_general(act, sc, turned, preferred_element_type=jnp.float32) * grad_scale
    repeats = n // groups
    input_grad = jnp.sum(home.reshape(repeats, groups * cap, width).astype(jnp.float32), axis=0)
    return input_grad, first[None], second[None]


def solution(mesh):
    in_specs = (
        P(("blk", "dp"), None),
        P(("blk", "dp"), None),
        P(("blk", "dp")),
        P(("blk", "dp"), None),
        P(),
        P("blk", None, None),
        P("blk", None, None),
    )
    out_specs = (P(("blk", "dp"), None), P("blk", "dp", None), P("blk", "dp", None))
    body = functools.partial(on_device, mesh.shape["blk"], mesh.shape["dp"])
    return jax.shard_map(body, mesh=mesh, in_specs=in_specs, out_specs=out_specs, check_vma=False)
```
